256 devices in a mesh: cuts: 32 (over z, x), mode: 8 (over y, core).
Axes of the slice: x: 4, y: 4, z: 8, core: 2. Of those that a mesh axis runs over, the one named last changes fastest.
Arguments:
- sliced_state: bfloat16 [8, 64, 4, 128, 2, 128], P(None, 'cuts', None, 'mode'), may hold values from -0.75 to 0.75
- gate_blocks: bfloat16 [32, 2, 128, 128], P('cuts'), may hold values from -0.375 to 0.375
- gate_slot: int32 [32], replicated, may hold values from 0 to 31, each once
- samples: int32 [8, 4096], replicated, may hold values from 0 to 65535
Outputs:
- amplitudes: float32 [32, 128, 2, 128], P('cuts', 'mode')
- sample_probs: float32 [8, 4096], replicated
- xeb_score: float32 [8], replicated
The draws below stay inside these ranges and needn't reach their ends.
Inputs may be any that keep to these rules, and one draw needn't show every extreme that they name: `gate_slot`: a permutation: every gate block has its own row of gate_blocks. `samples`: flat index s * 128 * 128 + p * 128 + q.
All inputs are finite; a program needn't handle non-finite values.
Results may differ from the reference program's by a relative error of at most 0.022.
Values may be sent and summed in bfloat16 or wider, within the bound.
A program may use at most 64 MiB of HBM per device.

```python
import jax
import jax.numpy as jnp

G = 128
S = 4
CIRC = 8
LAYERS = 2
SAMPLES = 4096
SLICES = 64
NBLK = 32


def plant(entries, rng, smallest, high):
    longest = entries.shape.index(max(entries.shape))
    spots = []
    for shift in (0, 1):
        where = [jax.random.randint(jax.random.fold_in(rng, axis), (), 0, length) for axis, length in enumerate(entries.shape)]
        where[longest] = (where[longest] + shift) % entries.shape[longest]
        spots.append(tuple(where))
    return entries.at[spots[0]].set(smallest).at[spots[1]].set(high)


def steps_of(own_key, extent, shards, smallest, high):
    level, own = 1.0, jax.random.fold_in(own_key, 6)
    for position, blocks in shards:
        steps = jnp.exp(jax.random.uniform(jax.random.fold_in(own, position), (blocks,), jnp.float32, smallest / len(shards), high / len(shards)))
        level = level * jnp.repeat(steps, extent[position] // blocks).reshape([-1 if axis == position else 1 for axis in range(len(extent))])
    return level


def bell_draw(stream_key, dims, deviation, most, split=(), held_as=jnp.bfloat16):
    level = steps_of(stream_key, dims, split, -0.22, 0.18) if split else 1.0
    array = jax.random.normal(stream_key, dims, jnp.float32) * deviation * level
    return jnp.minimum(jnp.maximum(array, -most), most).astype(held_as)


def setup_inputs(seed: int = 0) -> dict:
    arg_keys = jax.random.split(jax.random.key(seed), 5)
    return {
        "sliced_state": bell_draw(arg_keys[0], (CIRC, SLICES, S, G, 2, G), 0.125, 0.75, ((1, 32), (3, 8))),
        "gate_blocks": bell_draw(arg_keys[1], (NBLK, 2, G, G), (2 * G) ** -0.5, 0.375, ((0, 32),)),
        "gate_slot": jax.random.permutation(arg_keys[2], NBLK).astype(jnp.int32),
        "samples": plant(jax.random.randint(arg_keys[3], (CIRC, SAMPLES), 0, S * G * G), jax.random.fold_in(arg_keys[3], 1), 0, (S * G * G) - 1).astype(jnp.int32),
    }


def apply_gates(tensor, blocks):
    real_part = blocks[:, 0]
    imag_part = blocks[:, 1]
    stacked = jnp.concatenate([jnp.concatenate([real_part, imag_part], axis=2), jnp.concatenate([-imag_part, real_part], axis=2)], axis=1)
    layout = tensor.shape
    flattened = tensor.reshape(layout[0], -1, 2 * layout[-1])
    product = jnp.einsum("crk,ckn->crn", flattened.astype(jnp.float32), stacked.astype(jnp.float32))
    return product.astype(jnp.bfloat16).reshape(layout)


def reference(sliced_state, gate_blocks, gate_slot, samples):
    tensor = sliced_state
    circuit_ids = jnp.arange(CIRC, dtype=jnp.int32)
    for layer_index in range(LAYERS):
        for gate_kind in range(2):
            block_ids = (circuit_ids * LAYERS + layer_index) * 2 + gate_kind
            blocks = gate_blocks[gate_slot[block_ids]]
            if gate_kind == 1:
                tensor = jnp.swapaxes(tensor, 3, 5)
            tensor = apply_gates(tensor, blocks)
            if gate_kind == 1:
                tensor = jnp.swapaxes(tensor, 3, 5)
    amplitudes = jnp.sum(tensor.astype(jnp.float32), axis=1).reshape(CIRC * S, G, 2, G)
    magnitude = amplitudes[:, :, 0, :] ** 2 + amplitudes[:, :, 1, :] ** 2
    per_circuit = magnitude.reshape(CIRC, S * G * G)
    norm_total = jnp.sum(per_circuit, axis=1)
    picked = jnp.take_along_axis(per_circuit, samples, axis=1)
    sample_probs = picked * float(S * G * G) / norm_total[:, None]
    xeb_score = jnp.mean(sample_probs, axis=1)
    return amplitudes, sample_probs, xeb_score
```

```python
import jax
import jax.numpy as jnp
from jax import lax
from jax.experimental import pallas as pl
from jax.experimental.pallas import tpu as pltpu
from jax.sharding import Mesh
from jax.sharding import PartitionSpec as P

AXES = ("z", "x", "y", "core")
NZ, NX, NY, NC = 8, 4, 4, 2
ROWS = NZ * NX
PLANE = NX * NY * NC
G = 128
PP = G // (NY * NC)
MESH = pl.DeviceIdType.MESH
F32, BF16 = jnp.float32, jnp.bfloat16


def mm(a, b):
    return jnp.dot(a, b, preferred_element_type=F32)


def kernel(
    slot_ref, state_hbm, gates_hbm, samples_hbm, amp_ref, probs_ref, xeb_ref,
    state_v, gate_v, samp_v, part, rs, gr, sel, xs, msg, agg, agx, fin, prow, zbuf, tile,
    load_sem, send_sem, recv_sem,
):
    z, x, y, core = (lax.axis_index(name) for name in AXES)
    zx = z * NX + x
    pj = x * (NY * NC) + y * NC + core

    def zx_peer(k):
        return (lax.rem(z + k // NX, NZ), lax.rem(x + lax.rem(k, NX), NX), y, core)

    def plane_peer(k):
        dx, m = k // (NY * NC), lax.rem(k, NY * NC)
        return (z, lax.rem(x + dx, NX), lax.rem(y + m // NC, NY), lax.rem(core + lax.rem(m, NC), NC))

    def remote(src, dst, i, peer):
        return pltpu.make_async_remote_copy(
            src_ref=src, dst_ref=dst, send_sem=send_sem.at[i], recv_sem=recv_sem.at[i],
            device_id=peer, device_id_type=MESH,
        )

    def wait_bytes(ref, sem):
        pltpu.make_async_copy(ref, ref, sem).wait()

    chunk = pl.ds(pl.multiple_of(pj * G, G), G)
    load_gate = pltpu.make_async_copy(gates_hbm, gate_v, load_sem.at[0])
    load_state = pltpu.make_async_copy(state_hbm, state_v, load_sem.at[1])
    load_samp = pltpu.make_async_copy(samples_hbm.at[:, chunk], samp_v, load_sem.at[2])
    load_gate.start()
    load_state.start()
    load_samp.start()

    barrier = pltpu.get_barrier_semaphore()

    def greet(k, carry):
        pl.semaphore_signal(barrier, inc=1, device_id=zx_peer(k), device_id_type=MESH)
        pl.semaphore_signal(barrier, inc=1, device_id=plane_peer(k), device_id_type=MESH)
        return carry

    lax.fori_loop(1, 32, greet, 0)
    load_gate.wait()
    load_state.wait()
    for c in range(NZ):
        for s in range(NX):
            part[c * NX + s] = (state_v[c, 0, s].astype(F32) + state_v[c, 1, s].astype(F32)).astype(BF16)
    pl.semaphore_wait(barrier, 62)

    own_gate = pltpu.make_async_copy(gate_v.at[pj], gr.at[zx], recv_sem.at[0])
    own_gate.start()

    def send_gate(k, carry):
        peer = zx_peer(k)
        remote(gate_v.at[peer[1] * (NY * NC) + y * NC + core], gr.at[zx], 0, peer).start()
        return carry

    lax.fori_loop(1, ROWS, send_gate, 0)
    own_part = pltpu.make_async_copy(part.at[zx], rs.at[zx], recv_sem.at[1])
    own_part.start()

    def send_part(k, carry):
        peer = zx_peer(k)
        remote(part.at[peer[0] * NX + peer[1]], rs.at[zx], 1, peer).start()
        return carry

    lax.fori_loop(1, ROWS, send_part, 0)

    wait_bytes(gr, recv_sem.at[0])
    for g in range(4):
        sel[g] = gr[slot_ref[z * 4 + g]]
    own_sel = pltpu.make_async_copy(sel, agg.at[pj], recv_sem.at[2])
    own_sel.start()

    def send_sel(k, carry):
        remote(sel, agg.at[pj], 2, plane_peer(k)).start()
        return carry

    lax.fori_loop(1, PLANE, send_sel, 0)

    wait_bytes(rs, recv_sem.at[1])
    total = rs[0].astype(F32)
    for i in range(1, ROWS):
        total = total + rs[i].astype(F32)
    xs[...] = total
    msg[0:PP] = xs[pl.ds(0, PP, stride=2), :].astype(BF16)
    msg[PP : 2 * PP] = xs[pl.ds(1, PP, stride=2), :].astype(BF16)
    own_msg = pltpu.make_async_copy(msg, agx.at[pj], recv_sem.at[3])
    own_msg.start()

    def send_msg(k, carry):
        remote(msg, agx.at[pj], 3, plane_peer(k)).start()
        return carry

    lax.fori_loop(1, PLANE, send_msg, 0)

    wait_bytes(agg, recv_sem.at[2])

    def gate(g):
        both = agg[:, g].astype(F32).reshape(2 * G, G)
        return both[:G].astype(BF16), both[G:].astype(BF16)

    def product(first, second):
        (ar, ai), (br, bi) = first, second
        four = mm(jnp.concatenate([ar, ai], axis=0), jnp.concatenate([br, bi], axis=1))
        return four[:G, :G] - four[G:, G:], four[:G, G:] + four[G:, :G]

    qr, qi = product(gate(0), gate(2))
    pr, pi = product(gate(1), gate(3))
    q_mat = jnp.concatenate(
        [jnp.concatenate([qr, qi], axis=1), jnp.concatenate([-qi, qr], axis=1)], axis=0
    ).astype(BF16)
    prt, pit = pr.T, pi.T
    p_mat = jnp.concatenate(
        [jnp.concatenate([prt, -pit], axis=1), jnp.concatenate([pit, prt], axis=1)], axis=0
    ).astype(BF16)

    wait_bytes(agx, recv_sem.at[3])
    flat = jnp.concatenate(
        [agx[:, 0:PP].reshape(NX * G, G), agx[:, PP : 2 * PP].reshape(NX * G, G)], axis=1
    )
    turned = mm(flat, q_mat).astype(BF16)

    load_samp.wait()
    wanted = samp_v[pl.ds(z, 1), :]
    column = jnp.broadcast_to(wanted & (G - 1), (G, G))
    line = jnp.broadcast_to(wanted >> 7, (G, G))
    lines = lax.broadcasted_iota(jnp.int32, (G, G), 0)
    picked = jnp.zeros((G, G), F32)
    norms = jnp.zeros((G, G), F32)
    for s in range(NX):
        block = turned[s * G : (s + 1) * G]
        out = mm(p_mat, jnp.concatenate([block[:, :G], block[:, G:]], axis=0))
        fin[s] = out
        mag = out[:G] * out[:G] + out[G:] * out[G:]
        norms = norms + mag
        found = jnp.take_along_axis(mag, column, axis=1)
        picked = jnp.where(line == lines + s * G, found, picked)
    norm = jnp.sum(norms, axis=(0, 1), keepdims=True)
    mass = jnp.sum(picked, axis=0, keepdims=True)
    prow[0] = mass * float(NX * G * G) / norm

    own_row = pltpu.make_async_copy(prow.at[0], zbuf.at[z], recv_sem.at[4])
    own_row.start()

    def send_row(k, carry):
        remote(prow.at[0], zbuf.at[z], 4, (lax.rem(z + k, NZ), x, y, core)).start()
        return carry

    lax.fori_loop(1, NZ, send_row, 0)
    first = pl.multiple_of((y * NC + core) * PP, PP)
    amp_ref[pl.ds(0, PP, stride=2), :] = fin[x, pl.ds(first, PP), :]
    amp_ref[pl.ds(1, PP, stride=2), :] = fin[x, pl.ds(G + first, PP), :]
    wait_bytes(zbuf, recv_sem.at[4])
    for c in range(NZ):
        tile[pl.ds(c, 1), :] = zbuf[c]

    own_tile = pltpu.make_async_copy(tile, probs_ref.at[:, chunk], recv_sem.at[5])
    own_tile.start()

    def send_tile(k, carry):
        remote(tile, probs_ref.at[:, chunk], 5, plane_peer(k)).start()
        return carry

    lax.fori_loop(1, PLANE, send_tile, 0)
    wait_bytes(gr.at[pl.ds(0, ROWS - 1)], send_sem.at[0])
    wait_bytes(rs.at[pl.ds(0, ROWS - 1)], send_sem.at[1])
    wait_bytes(agg.at[pl.ds(0, PLANE - 1)], send_sem.at[2])
    wait_bytes(agx.at[pl.ds(0, PLANE - 1)], send_sem.at[3])
    wait_bytes(zbuf.at[pl.ds(0, NZ - 1)], send_sem.at[4])
    wait_bytes(probs_ref, recv_sem.at[5])
    wait_bytes(probs_ref.at[:, pl.ds(0, G * (PLANE - 1))], send_sem.at[5])
    means = jnp.sum(probs_ref[...], axis=1, keepdims=True) * (1.0 / (PLANE * G))
    spot = lax.broadcasted_iota(jnp.int32, (NZ, G), 0) == lax.broadcasted_iota(jnp.int32, (NZ, G), 1)
    xeb_ref[...] = jnp.sum(jnp.where(spot, means, 0.0), axis=0, keepdims=True)


def on_device(sliced_state, gate_blocks, gate_slot, samples):
    state = sliced_state.reshape(NZ, 2, NX, 2 * PP, G)
    gates = gate_blocks.reshape(PLANE, 8, G)
    vmem, hbm = pl.BlockSpec(memory_space=pltpu.VMEM), pl.BlockSpec(memory_space=pl.ANY)
    amp, probs, xeb = pl.pallas_call(
        kernel,
        out_shape=(
            jax.ShapeDtypeStruct((2 * PP, G), F32),
            jax.ShapeDtypeStruct((NZ, PLANE * G), F32),
            jax.ShapeDtypeStruct((1, G), F32),
        ),
        in_specs=[pl.BlockSpec(memory_space=pltpu.SMEM), hbm, hbm, hbm],
        out_specs=(vmem, vmem, vmem),
        scratch_shapes=[
            pltpu.VMEM((NZ, 2, NX, 2 * PP, G), BF16),
            pltpu.VMEM((PLANE, 8, G), BF16),
            pltpu.VMEM((NZ, G), jnp.int32),
            pltpu.VMEM((ROWS, 2 * PP, G), BF16),
            pltpu.VMEM((ROWS, 2 * PP, G), BF16),
            pltpu.VMEM((ROWS, 8, G), BF16),
            pltpu.VMEM((4, 8, G), BF16),
            pltpu.VMEM((2 * PP, G), F32),
            pltpu.VMEM((2 * PP, G), BF16),
            pltpu.VMEM((PLANE, 4, 8, G), BF16),
            pltpu.VMEM((PLANE, 2 * PP, G), BF16),
            pltpu.VMEM((NX, 2 * G, G), F32),
            pltpu.VMEM((1, 1, G), F32),
            pltpu.VMEM((NZ, 1, G), F32),
            pltpu.VMEM((NZ, G), F32),
            pltpu.SemaphoreType.DMA((3,)),
            pltpu.SemaphoreType.DMA((6,)),
            pltpu.SemaphoreType.DMA((6,)),
        ],
        compiler_params=pltpu.CompilerParams(collective_id=0, has_side_effects=True),
        name="amplitudes",
    )(gate_slot, state, gates, samples)
    return amp.reshape(1, PP, 2, G), probs, xeb[0, :NZ]


def solution(mesh):
    split = Mesh(mesh.devices.reshape(NZ, NX, NY, NC), AXES)
    cuts, mode = ("z", "x"), ("y", "core")
    return jax.shard_map(
        on_device,
        mesh=split,
        in_specs=(P(None, cuts, None, mode, None, None), P(cuts, None, None, None), P(), P()),
        out_specs=(P(cuts, mode, None, None), P(), P()),
        check_vma=False,
    )
```

```python
import jax
import jax.numpy as jnp
from jax import lax
from jax.experimental import pallas as pl
from jax.experimental.pallas import tpu as pltpu
from jax.sharding import Mesh
from jax.sharding import PartitionSpec as P

AXES = ("z", "x", "y", "core")
NZ, NX, NY, NC = 8, 4, 4, 2
ROWS = NZ * NX
CHIPS = NX * NY
PLANE = CHIPS * NC
G = 128
PP = G // (NY * NC)
CHUNKS = 4096 // G // NC
MESH = pl.DeviceIdType.MESH
F32, BF16 = jnp.float32, jnp.bfloat16


def hops(offset):
    return sum(min(d, n - d) for d, n in zip(offset, (NZ, NX, NY, NC)))


def far_first(offsets):
    return sorted((o for o in offsets if any(o)), key=hops, reverse=True)


OVER_CUTS = far_first([(dz, dx, 0, 0) for dz in range(NZ) for dx in range(NX)])
IN_PLANE = far_first([(0, dx, dy, dc) for dx in range(NX) for dy in range(NY) for dc in range(NC)])
SAME_CORE = [o for o in IN_PLANE if o[3] == 0]
OVER_X = far_first([(0, dx, 0, 0) for dx in range(NX)])
OVER_Z = far_first([(dz, 0, 0, 0) for dz in range(NZ)])
GREETED = far_first(set(OVER_CUTS) | set(IN_PLANE))
PARTNER = (0, 0, 0, 1)
GATE, SEL, SWAP, SUMS, LINES, PROBS, HALF, FIRST = range(8)


def mm(a, b):
    return jnp.dot(a, b, preferred_element_type=F32)


def scope(name):
    return jax.named_scope(name)


def exchange(
    slot_hbm, state_hbm, gates_hbm, samples_hbm, amp_ref, probs_ref,
    slot_s, state_v, gate_v, samp_v, asked, part, xr, zs, zr, gr, sel, agg, xs, msg, agx, fin, mags, prow, zbuf,
    load_sem, send_sem, recv_sem,
):
    at = [lax.axis_index(name) for name in AXES]
    turn = [[i] + [lax.rem(i + d, n) for d in range(1, n)] for i, n in zip(at, (NZ, NX, NY, NC))]
    z, x, y, core = at
    zx, chip = z * NX + x, x * NY + y

    def peer(offset):
        return tuple(turn[axis][d] for axis, d in enumerate(offset))

    def send(src, dst, i, offset, j=None):
        pltpu.make_async_remote_copy(
            src_ref=src, dst_ref=dst, send_sem=send_sem.at[i], recv_sem=recv_sem.at[i if j is None else j],
            device_id=peer(offset), device_id_type=MESH,
        ).start()

    def keep(src, dst, i):
        pltpu.make_async_copy(src, dst, recv_sem.at[i]).start()

    def wait_bytes(ref, sem):
        pltpu.make_async_copy(ref, ref, sem).wait()

    with scope("greet"):
        load_state = pltpu.make_async_copy(state_hbm, state_v, load_sem.at[0])
        load_gate = pltpu.make_async_copy(gates_hbm, gate_v, load_sem.at[1])
        load_slot = pltpu.make_async_copy(slot_hbm, slot_s, load_sem.at[2])
        half = pl.ds(pl.multiple_of(core * CHUNKS * G, G), CHUNKS * G)
        load_samp = pltpu.make_async_copy(samples_hbm.at[:, half], samp_v, load_sem.at[3])
        for load in (load_state, load_gate, load_slot, load_samp):
            load.start()
        barrier = pltpu.get_barrier_semaphore()
        for offset in GREETED:
            pl.semaphore_signal(barrier, inc=1, device_id=peer(offset), device_id_type=MESH)
    with scope("sum"):
        load_state.wait()
        for c in range(NZ):
            for s in range(NX):
                part[c, s] = (state_v[c, 0, s].astype(F32) + state_v[c, 1, s].astype(F32)).astype(BF16)
        load_gate.wait()
    with scope("barrier"):
        pl.semaphore_wait(barrier, len(GREETED))

    with scope("send_a"):
        for offset in OVER_CUTS:
            _, px, _, _ = peer(offset)
            send(gate_v.at[core * CHIPS + px * NY + y], gr.at[zx], GATE, offset)
        order = [dz for dz, *_ in OVER_Z] + [0]
        for i, dz in enumerate(order):
            for offset in OVER_X:
                dx = offset[1]
                send(part.at[turn[0][dz], turn[1][dx]], xr.at[i, dx - 1], FIRST, offset, FIRST + i)
        keep(gate_v.at[core * CHIPS + chip], gr.at[zx], GATE)
    own = None
    for i, dz in enumerate(order):
        with scope("sums_%d" % i):
            wait_bytes(xr.at[i], recv_sem.at[FIRST + i])
            own = part[turn[0][dz], x].astype(F32)
            for dx in range(1, NX):
                own = own + xr[i, dx - 1].astype(F32)
            if dz:
                zs[i] = own.astype(BF16)
                send(zs.at[i], zr.at[dz - 1], SUMS, OVER_Z[i])

    with scope("wait_gate"):
        load_slot.wait()
        wait_bytes(gr, recv_sem.at[GATE])
    with scope("send_sel"):
        for g in range(4):
            sel[g] = gr[slot_s[z * 4 + g]]
        for offset in SAME_CORE:
            send(sel, agg.at[core, chip], SEL, offset)
        keep(sel, agg.at[core, chip], SEL)
    with scope("wait_sums"):
        wait_bytes(zr, recv_sem.at[SUMS])
    with scope("send_lines"):
        for i in range(NZ - 1):
            own = own + zr[i].astype(F32)
        xs[...] = own
        msg[0:PP] = xs[pl.ds(0, PP, stride=2), :].astype(BF16)
        msg[PP : 2 * PP] = xs[pl.ds(1, PP, stride=2), :].astype(BF16)
        place = chip * NC + core
        for offset in IN_PLANE:
            send(msg, agx.at[place], LINES, offset)
        keep(msg, agx.at[place], LINES)
    with scope("wait_sel"):
        wait_bytes(agg.at[0], recv_sem.at[SEL])
    with scope("swap"):
        send(agg.at[core], agg.at[core], SWAP, PARTNER)
        wait_bytes(agg.at[0], recv_sem.at[SWAP])

    def gate(g):
        both = agg[:, :, g].astype(F32).reshape(2 * G, G)
        return both[:G].astype(BF16), both[G:].astype(BF16)

    def product(first, second):
        (ar, ai), (br, bi) = first, second
        four = mm(jnp.concatenate([ar, ai], axis=0), jnp.concatenate([br, bi], axis=1))
        return four[:G, :G] - four[G:, G:], four[:G, G:] + four[G:, :G]

    with scope("mats"):
        qr, qi = product(gate(0), gate(2))
        pr, pi = product(gate(1), gate(3))
        q_mat = jnp.concatenate(
            [jnp.concatenate([qr, qi], axis=1), jnp.concatenate([-qi, qr], axis=1)], axis=0
        ).astype(BF16)
        prt, pit = pr.T, pi.T
        p_mat = jnp.concatenate(
            [jnp.concatenate([prt, -pit], axis=1), jnp.concatenate([pit, prt], axis=1)], axis=0
        ).astype(BF16)
    with scope("wait_lines"):
        load_samp.wait()
        for k in range(CHUNKS):
            asked[k] = samp_v[:, k * G : (k + 1) * G]
        wait_bytes(agx, recv_sem.at[LINES])
    with scope("math"):
        flat = jnp.concatenate(
            [agx[:, 0:PP].reshape(NX * G, G), agx[:, PP : 2 * PP].reshape(NX * G, G)], axis=1
        )
        turned = mm(flat, q_mat).astype(BF16)
        norms = jnp.zeros((G, G), F32)
        for s in range(NX):
            block = turned[s * G : (s + 1) * G]
            out = mm(p_mat, jnp.concatenate([block[:, :G], block[:, G:]], axis=0))
            fin[s] = out
            mag = out[:G] * out[:G] + out[G:] * out[G:]
            mags[s * G : (s + 1) * G] = mag
            norms = norms + mag
        scale = float(NX * G * G) / jnp.sum(norms, axis=(0, 1), keepdims=True)
    with scope("look_up"):
        lines = lax.broadcasted_iota(jnp.int32, (8, G), 0)
        for k in range(CHUNKS):
            wanted = asked[k, pl.ds(z, 1), :]
            column = jnp.broadcast_to(wanted & (G - 1), (8, G))
            line = jnp.broadcast_to(wanted >> 7, (8, G)) - lines
            picked = jnp.zeros((8, G), F32)
            for r in range(0, NX * G, 8):
                found = jnp.take_along_axis(mags[r : r + 8], column, axis=1)
                picked = jnp.where(line == r, found, picked)
            prow[k : k + 1] = jnp.sum(picked, axis=0, keepdims=True) * scale

    with scope("send_c"):
        for offset in OVER_Z:
            send(prow, zbuf.at[z], PROBS, offset)
        keep(prow, zbuf.at[z], PROBS)
        first = pl.multiple_of((y * NC + core) * PP, PP)
        amp_ref[pl.ds(0, PP, stride=2), :] = fin[x, pl.ds(first, PP), :]
        amp_ref[pl.ds(1, PP, stride=2), :] = fin[x, pl.ds(G + first, PP), :]
        wait_bytes(gr.at[pl.ds(0, ROWS - 1)], send_sem.at[GATE])
        wait_bytes(xr, send_sem.at[FIRST])
        wait_bytes(zr, send_sem.at[SUMS])
        wait_bytes(agg.at[0, pl.ds(0, CHIPS - 1)], send_sem.at[SEL])
        wait_bytes(agg.at[0], send_sem.at[SWAP])
        wait_bytes(agx.at[pl.ds(0, PLANE - 1)], send_sem.at[LINES])
        wait_bytes(zbuf.at[pl.ds(0, NZ - 1)], send_sem.at[PROBS])
    with scope("wait_c"):
        wait_bytes(zbuf, recv_sem.at[PROBS])
    with scope("send_d"):
        for c in range(NZ):
            probs_ref[core, c] = zbuf[c]
        send(probs_ref.at[core], probs_ref.at[core], HALF, PARTNER)
    with scope("wait_d"):
        wait_bytes(probs_ref.at[0], recv_sem.at[HALF])
        wait_bytes(probs_ref.at[0], send_sem.at[HALF])


def hand_out(amp_v, probs_v, amp_hbm, probs_hbm, xeb_ref, lined, sem):
    keep_amp = pltpu.make_async_copy(amp_v, amp_hbm, sem.at[0])
    keep_amp.start()
    total = jnp.zeros((NZ, G), F32)
    for half in range(NC):
        for k in range(CHUNKS):
            run = jnp.concatenate([probs_v[half, c, k : k + 1] for c in range(NZ)], axis=0)
            lined[:, (half * CHUNKS + k) * G : (half * CHUNKS + k + 1) * G] = run
            total = total + run
    keep_probs = pltpu.make_async_copy(lined, probs_hbm, sem.at[1])
    keep_probs.start()
    means = jnp.sum(total, axis=1, keepdims=True) * (1.0 / (NC * CHUNKS * G))
    spot = lax.broadcasted_iota(jnp.int32, (NZ, G), 0) == lax.broadcasted_iota(jnp.int32, (NZ, G), 1)
    xeb_ref[...] = jnp.sum(jnp.where(spot, means, 0.0), axis=0, keepdims=True)[:, :NZ]
    keep_amp.wait()
    keep_probs.wait()


def on_device(sliced_state, gate_blocks, gate_slot, samples):
    state = sliced_state.reshape(NZ, 2, NX, 2 * PP, G)
    gates = gate_blocks.reshape(PLANE, 8, G)
    hbm, vmem = pl.BlockSpec(memory_space=pl.ANY), pl.BlockSpec(memory_space=pltpu.VMEM)
    block = (2 * PP, G)
    amp, probs = pl.pallas_call(
        exchange,
        out_shape=(pltpu.VMEM(block, F32), pltpu.VMEM((NC, NZ, CHUNKS, G), F32)),
        in_specs=[hbm] * 4,
        out_specs=(vmem, vmem),
        scratch_shapes=[
            pltpu.SMEM((ROWS,), jnp.int32),
            pltpu.VMEM((NZ, 2, NX) + block, BF16),
            pltpu.VMEM((PLANE, 8, G), BF16),
            pltpu.VMEM((NZ, CHUNKS * G), jnp.int32),
            pltpu.VMEM((CHUNKS, NZ, G), jnp.int32),
            pltpu.VMEM((NZ, NX) + block, BF16),
            pltpu.VMEM((NZ, NX - 1) + block, BF16),
            pltpu.VMEM((NZ - 1,) + block, BF16),
            pltpu.VMEM((NZ - 1,) + block, BF16),
            pltpu.VMEM((ROWS, 8, G), BF16),
            pltpu.VMEM((4, 8, G), BF16),
            pltpu.VMEM((NC, CHIPS, 4, 8, G), BF16),
            pltpu.VMEM(block, F32),
            pltpu.VMEM(block, BF16),
            pltpu.VMEM((PLANE,) + block, BF16),
            pltpu.VMEM((NX, 2 * G, G), F32),
            pltpu.VMEM((NX * G, G), F32),
            pltpu.VMEM((CHUNKS, G), F32),
            pltpu.VMEM((NZ, CHUNKS, G), F32),
            pltpu.SemaphoreType.DMA((4,)),
            pltpu.SemaphoreType.DMA((FIRST + NZ,)),
            pltpu.SemaphoreType.DMA((FIRST + NZ,)),
        ],
        compiler_params=pltpu.CompilerParams(collective_id=0, has_side_effects=True),
        name="amplitudes",
    )(gate_slot, state, gates, samples)
    amp, probs, xeb = pl.pallas_call(
        hand_out,
        out_shape=(
            jax.ShapeDtypeStruct(block, F32),
            jax.ShapeDtypeStruct((NZ, NC * CHUNKS * G), F32),
            jax.ShapeDtypeStruct((1, NZ), F32),
        ),
        in_specs=[vmem, vmem],
        out_specs=(hbm, hbm, vmem),
        scratch_shapes=[pltpu.VMEM((NZ, NC * CHUNKS * G), F32), pltpu.SemaphoreType.DMA((2,))],
        name="hand_out",
    )(*(pltpu.with_memory_space_constraint(array, pltpu.VMEM) for array in (amp, probs)))
    return amp.reshape(1, PP, 2, G), probs, xeb.reshape(NZ)


def solution(mesh):
    split = Mesh(mesh.devices.reshape(NZ, NX, NY, NC), AXES)
    cuts, mode = ("z", "x"), ("y", "core")
    return jax.shard_map(
        on_device,
        mesh=split,
        in_specs=(P(None, cuts, None, mode, None, None), P(cuts, None, None, None), P(), P()),
        out_specs=(P(cuts, mode, None, None), P(), P()),
        check_vma=False,
    )
```

```python
import jax
import jax.numpy as jnp
from jax import lax
from jax.experimental import pallas as pl
from jax.experimental.pallas import tpu as pltpu
from jax.sharding import Mesh
from jax.sharding import PartitionSpec as P

AXES = ("z", "x", "y", "core")
NZ, NX, NY, NC = 8, 4, 4, 2
ROWS = NZ * NX
CHIPS = NX * NY
PLANE = CHIPS * NC
G = 128
PP = G // (NY * NC)
RUNS = 4096 // G
MESH = pl.DeviceIdType.MESH
F32, BF16 = jnp.float32, jnp.bfloat16


def hops(offset):
    return sum(min(d, n - d) for d, n in zip(offset, (NZ, NX, NY, NC)))


def far_first(offsets):
    return sorted((o for o in offsets if any(o)), key=hops, reverse=True)


IN_PLANE = far_first([(0, dx, dy, dc) for dx in range(NX) for dy in range(NY) for dc in range(NC)])
SAME_CORE = [o for o in IN_PLANE if o[3] == 0]
OVER_X = far_first([(0, dx, 0, 0) for dx in range(NX)])
OVER_Z = far_first([(dz, 0, 0, 0) for dz in range(NZ)])
NEAR = [o for o in SAME_CORE if hops(o) <= 2]
DIRECT = [o for o in IN_PLANE if o[:3] not in [n[:3] for n in NEAR]]
GREETED = far_first(set(OVER_Z) | set(IN_PLANE))
PARTNER = (0, 0, 0, 1)
PIECE, GATE, SEL, SWAP, SUMS, CLOSE, LINES, PROBS, FIRST = range(9)


def mm(a, b):
    return jnp.dot(a, b, preferred_element_type=F32)


def scope(name):
    return jax.named_scope(name)


def exchange(
    slot_hbm, state_hbm, gates_hbm, samples_hbm, amp_ref, probs_ref,
    slot_s, state_v, gate_v, samp_v, asked, hot, part, xr, zs, zr, gx, gr, sel, agg, xs, msg, agx, fin, mags, rows, prow,
    load_sem, send_sem, recv_sem,
):
    at = [lax.axis_index(name) for name in AXES]
    turn = [[i] + [lax.rem(i + d, n) for d in range(1, n)] for i, n in zip(at, (NZ, NX, NY, NC))]
    z, x, y, core = at
    chip = x * NY + y

    def peer(offset):
        return tuple(turn[axis][d] for axis, d in enumerate(offset))

    def send(src, dst, i, offset, j=None):
        pltpu.make_async_remote_copy(
            src_ref=src, dst_ref=dst, send_sem=send_sem.at[i], recv_sem=recv_sem.at[i if j is None else j],
            device_id=peer(offset), device_id_type=MESH,
        ).start()

    def keep(src, dst, i):
        pltpu.make_async_copy(src, dst, recv_sem.at[i]).start()

    def wait_bytes(ref, sem):
        pltpu.make_async_copy(ref, ref, sem).wait()

    with scope("greet"):
        load_state = pltpu.make_async_copy(state_hbm, state_v, load_sem.at[0])
        load_gate = pltpu.make_async_copy(gates_hbm, gate_v, load_sem.at[1])
        load_slot = pltpu.make_async_copy(slot_hbm, slot_s, load_sem.at[2])
        load_samp = pltpu.make_async_copy(samples_hbm, samp_v, load_sem.at[3])
        for load in (load_state, load_gate, load_slot, load_samp):
            load.start()
        barrier = pltpu.get_barrier_semaphore()
        for offset in GREETED:
            pl.semaphore_signal(barrier, inc=1, device_id=peer(offset), device_id_type=MESH)
    with scope("sum"):
        load_state.wait()
        for c in range(NZ):
            for s in range(NX):
                part[c, s] = (state_v[c, 0, s].astype(F32) + state_v[c, 1, s].astype(F32)).astype(BF16)
        load_gate.wait()
    with scope("barrier"):
        pl.semaphore_wait(barrier, len(GREETED))

    with scope("send_a"):
        for offset in OVER_X:
            px = peer(offset)[1]
            send(gate_v.at[core * CHIPS + px * NY + y], gx.at[x], PIECE, offset)
        keep(gate_v.at[core * CHIPS + chip], gx.at[x], PIECE)
        order = [dz for dz, *_ in OVER_Z] + [0]
        for i, dz in enumerate(order):
            for offset in OVER_X:
                dx = offset[1]
                send(part.at[turn[0][dz], turn[1][dx]], xr.at[i, dx - 1], FIRST, offset, FIRST + i)
    with scope("send_gx"):
        held = gr.at[pl.ds(z * NX, NX)]
        wait_bytes(gx, recv_sem.at[PIECE])
        for offset in OVER_Z:
            send(gx, held, GATE, offset)
        keep(gx, held, GATE)
    own = None
    for i, dz in enumerate(order):
        with scope("sums_%d" % i):
            wait_bytes(xr.at[i], recv_sem.at[FIRST + i])
            own = part[turn[0][dz], x].astype(F32)
            for dx in range(1, NX):
                own = own + xr[i, dx - 1].astype(F32)
            if dz:
                zs[i] = own.astype(BF16)
                send(zs.at[i], zr.at[dz - 1], SUMS, OVER_Z[i])

    with scope("wait_gate"):
        load_slot.wait()
        wait_bytes(gr, recv_sem.at[GATE])
    with scope("send_sel"):
        for g in range(4):
            sel[g] = gr[slot_s[z * 4 + g]]
        for offset in SAME_CORE:
            send(sel, agg.at[core, chip], SEL, offset)
        keep(sel, agg.at[core, chip], SEL)
    with scope("wait_sums"):
        wait_bytes(zr, recv_sem.at[SUMS])
    with scope("send_lines"):
        for i in range(NZ - 1):
            own = own + zr[i].astype(F32)
        xs[...] = own
        msg[0:PP] = xs[pl.ds(0, PP, stride=2), :].astype(BF16)
        msg[PP : 2 * PP] = xs[pl.ds(1, PP, stride=2), :].astype(BF16)
        place = chip * NC + core
        for offset in DIRECT:
            send(msg, agx.at[place], LINES, offset)
        for offset in NEAR:
            send(msg, agx.at[place], CLOSE, offset)
        keep(msg, agx.at[place], LINES)
    with scope("one_hot"):
        load_samp.wait()
        for k in range(RUNS):
            asked[k] = samp_v[:, k * G : (k + 1) * G]
        places = lax.broadcasted_iota(jnp.int32, (2 * G, G), 0)
        for k in range(RUNS):
            wanted = asked[k, pl.ds(z, 1), :]
            column = (wanted & (G - 1)) + ((wanted >> 15) << 7)
            hot[:, k * G : (k + 1) * G] = jnp.where(column == places, 1.0, 0.0).astype(BF16)
    with scope("wait_sel"):
        wait_bytes(agg.at[0], recv_sem.at[SEL])
    with scope("swap"):
        send(agg.at[core], agg.at[core], SWAP, PARTNER)
    with scope("hand_over"):
        close = agx.at[pl.ds(0, len(NEAR))]
        wait_bytes(close, recv_sem.at[CLOSE])
        for offset in NEAR:
            _, px, py, _ = peer(offset)
            passed = agx.at[(px * NY + py) * NC + core]
            send(passed, passed, LINES, PARTNER)
    with scope("wait_swap"):
        wait_bytes(agg.at[0], recv_sem.at[SWAP])

    def gate(g):
        both = agg[:, :, g].astype(F32).reshape(2 * G, G)
        return both[:G].astype(BF16), both[G:].astype(BF16)

    def product(first, second):
        (ar, ai), (br, bi) = first, second
        four = mm(jnp.concatenate([ar, ai], axis=0), jnp.concatenate([br, bi], axis=1))
        return four[:G, :G] - four[G:, G:], four[:G, G:] + four[G:, :G]

    with scope("mats"):
        qr, qi = product(gate(0), gate(2))
        pr, pi = product(gate(1), gate(3))
        q_mat = jnp.concatenate(
            [jnp.concatenate([qr, qi], axis=1), jnp.concatenate([-qi, qr], axis=1)], axis=0
        ).astype(BF16)
        prt, pit = pr.T, pi.T
        p_mat = jnp.concatenate(
            [jnp.concatenate([prt, -pit], axis=1), jnp.concatenate([pit, prt], axis=1)], axis=0
        ).astype(BF16)
    with scope("wait_lines"):
        wait_bytes(agx.at[pl.ds(0, PLANE - len(NEAR))], recv_sem.at[LINES])
    with scope("math"):
        flat = jnp.concatenate(
            [agx[:, 0:PP].reshape(NX * G, G), agx[:, PP : 2 * PP].reshape(NX * G, G)], axis=1
        )
        turned = mm(flat, q_mat).astype(BF16)
        norms = jnp.zeros((G, G), F32)
        for s in range(NX):
            block = turned[s * G : (s + 1) * G]
            out = mm(p_mat, jnp.concatenate([block[:, :G], block[:, G:]], axis=0))
            fin[s] = out
            mag = out[:G] * out[:G] + out[G:] * out[G:]
            mags[s * G : (s + 1) * G] = mag
            norms = norms + mag
        scale = float(NX * G * G) / jnp.sum(norms, axis=(0, 1), keepdims=True)
    with scope("look_up"):
        table = (mags[...] * scale).astype(BF16)
        pairs = jnp.concatenate([table[: 2 * G], table[2 * G :]], axis=1)
        lines = lax.broadcasted_iota(jnp.int32, (2 * G, G), 0)
    for part_of, runs in ((0, range(RUNS // 2)), (1, range(RUNS // 2, RUNS))):
        with scope("look_up_%d" % part_of):
            for k in runs:
                found = mm(pairs, hot[:, k * G : (k + 1) * G])
                line = (asked[k, pl.ds(z, 1), :] >> 7) & (2 * G - 1)
                rows[k : k + 1] = jnp.sum(jnp.where(line == lines, found, 0.0), axis=0, keepdims=True)
            some = pl.ds(part_of * RUNS // 2, RUNS // 2)
            prow[part_of] = rows[some, :].astype(BF16)
            for offset in OVER_Z:
                send(prow.at[part_of], probs_ref.at[z, some], PROBS, offset)
            keep(prow.at[part_of], probs_ref.at[z, some], PROBS)
    with scope("clear"):
        first = pl.multiple_of((y * NC + core) * PP, PP)
        amp_ref[pl.ds(0, PP, stride=2), :] = fin[x, pl.ds(first, PP), :]
        amp_ref[pl.ds(1, PP, stride=2), :] = fin[x, pl.ds(G + first, PP), :]
        wait_bytes(gx.at[pl.ds(0, NX - 1)], send_sem.at[PIECE])
        wait_bytes(gr.at[pl.ds(0, ROWS - NX)], send_sem.at[GATE])
        wait_bytes(xr, send_sem.at[FIRST])
        wait_bytes(zr, send_sem.at[SUMS])
        wait_bytes(agg.at[0, pl.ds(0, CHIPS - 1)], send_sem.at[SEL])
        wait_bytes(agg.at[0], send_sem.at[SWAP])
        wait_bytes(close, send_sem.at[CLOSE])
        wait_bytes(agx.at[pl.ds(0, len(DIRECT) + len(NEAR))], send_sem.at[LINES])
    with scope("wait_c"):
        wait_bytes(probs_ref, recv_sem.at[PROBS])
        wait_bytes(probs_ref.at[pl.ds(0, NZ - 1)], send_sem.at[PROBS])


def hand_out(amp_v, probs_v, amp_hbm, probs_hbm, xeb_ref, wide, lined, sem):
    keep_amp = pltpu.make_async_copy(amp_v, amp_hbm, sem.at[0])
    keep_amp.start()
    wide[...] = probs_v[...].astype(F32).reshape(NZ * RUNS, G)
    total = jnp.zeros((NZ, G), F32)
    for k in range(RUNS):
        run = wide[pl.ds(k, NZ, stride=RUNS), :]
        lined[:, k * G : (k + 1) * G] = run
        total = total + run
    keep_probs = pltpu.make_async_copy(lined, probs_hbm, sem.at[1])
    keep_probs.start()
    means = jnp.sum(total, axis=1, keepdims=True) * (1.0 / (RUNS * G))
    spot = lax.broadcasted_iota(jnp.int32, (NZ, G), 0) == lax.broadcasted_iota(jnp.int32, (NZ, G), 1)
    xeb_ref[...] = jnp.sum(jnp.where(spot, means, 0.0), axis=0, keepdims=True)[:, :NZ]
    keep_amp.wait()
    keep_probs.wait()


def on_device(sliced_state, gate_blocks, gate_slot, samples):
    state = sliced_state.reshape(NZ, 2, NX, 2 * PP, G)
    gates = gate_blocks.reshape(PLANE, 8, G)
    hbm, vmem = pl.BlockSpec(memory_space=pl.ANY), pl.BlockSpec(memory_space=pltpu.VMEM)
    block = (2 * PP, G)
    amp, probs = pl.pallas_call(
        exchange,
        out_shape=(pltpu.VMEM(block, F32), pltpu.VMEM((NZ, RUNS, G), BF16)),
        in_specs=[hbm] * 4,
        out_specs=(vmem, vmem),
        scratch_shapes=[
            pltpu.SMEM((ROWS,), jnp.int32),
            pltpu.VMEM((NZ, 2, NX) + block, BF16),
            pltpu.VMEM((PLANE, 8, G), BF16),
            pltpu.VMEM((NZ, RUNS * G), jnp.int32),
            pltpu.VMEM((RUNS, NZ, G), jnp.int32),
            pltpu.VMEM((2 * G, RUNS * G), BF16),
            pltpu.VMEM((NZ, NX) + block, BF16),
            pltpu.VMEM((NZ, NX - 1) + block, BF16),
            pltpu.VMEM((NZ - 1,) + block, BF16),
            pltpu.VMEM((NZ - 1,) + block, BF16),
            pltpu.VMEM((NX, 8, G), BF16),
            pltpu.VMEM((ROWS, 8, G), BF16),
            pltpu.VMEM((4, 8, G), BF16),
            pltpu.VMEM((NC, CHIPS, 4, 8, G), BF16),
            pltpu.VMEM(block, F32),
            pltpu.VMEM(block, BF16),
            pltpu.VMEM((PLANE,) + block, BF16),
            pltpu.VMEM((NX, 2 * G, G), F32),
            pltpu.VMEM((NX * G, G), F32),
            pltpu.VMEM((RUNS, G), F32),
            pltpu.VMEM((2, RUNS // 2, G), BF16),
            pltpu.SemaphoreType.DMA((4,)),
            pltpu.SemaphoreType.DMA((FIRST + NZ,)),
            pltpu.SemaphoreType.DMA((FIRST + NZ,)),
        ],
        compiler_params=pltpu.CompilerParams(collective_id=0, has_side_effects=True),
        name="amplitudes",
    )(gate_slot, state, gates, samples)
    amp, probs, xeb = pl.pallas_call(
        hand_out,
        out_shape=(
            jax.ShapeDtypeStruct(block, F32),
            jax.ShapeDtypeStruct((NZ, RUNS * G), F32),
            jax.ShapeDtypeStruct((1, NZ), F32),
        ),
        in_specs=[vmem, vmem],
        out_specs=(hbm, hbm, vmem),
        scratch_shapes=[
            pltpu.VMEM((NZ * RUNS, G), F32),
            pltpu.VMEM((NZ, RUNS * G), F32),
            pltpu.SemaphoreType.DMA((2,)),
        ],
        name="hand_out",
    )(*(pltpu.with_memory_space_constraint(array, pltpu.VMEM) for array in (amp, probs)))
    return amp.reshape(1, PP, 2, G), probs, xeb.reshape(NZ)


def solution(mesh):
    split = Mesh(mesh.devices.reshape(NZ, NX, NY, NC), AXES)
    cuts, mode = ("z", "x"), ("y", "core")
    return jax.shard_map(
        on_device,
        mesh=split,
        in_specs=(P(None, cuts, None, mode, None, None), P(cuts, None, None, None), P(), P()),
        out_specs=(P(cuts, mode, None, None), P(), P()),
        check_vma=False,
    )
```
